32 devices in a mesh: rows: 8 (over z, x), cols: 4 (over y, core).
Axes of the slice: x: 2, y: 2, z: 4, core: 2. Of those that a mesh axis runs over, the one named last changes fastest.
Arguments:
- basis: float32 [8192, 4096], P('rows', 'cols'), may hold values from -119.66257 to 119.66257, as said below
- block: float32 [8192, 512], P('rows', 'cols'), may hold values from -1800 to 1800
Outputs:
- ortho: float32 [8192, 512], P('rows', 'cols')
- factors: float32 [4, 128, 128], P('cols')
The draws below stay inside these ranges and needn't reach their ends.
Inputs may be any that keep to these rules, and one draw needn't show every extreme that they name: Under the inner product (sum over rows divided by 8192) the basis columns have squared norms between 0.6 and 1.9, and inner products of distinct basis columns are at most 0.05 in magnitude.
All inputs are finite; a program needn't handle non-finite values.
Results may differ from the reference program's by a relative error of at most 0.000076.
Values sent between devices are 32-bit elements; how exact they have to be, the bound alone decides.
No kernel may reach another device: no remote copies, remote signals or barrier semaphores. Data moves between devices by JAX's collectives and lax.ppermute only.
A program may use at most 64 MiB of HBM per device.

```python
import math
import jax
import jax.numpy as jnp
from jax import lax

K = 4096
BLK = 128
NBLK = 4
M = 8192


def draw_basis(key, part):
    keys = jax.random.split(key, 8)
    group = 128
    chosen = jax.random.permutation(keys[0], M)[:K]
    field = (jnp.arange(M, dtype=jnp.int32)[:, None] == chosen[None, :]).astype(jnp.float32)
    for section in range(3):
        order = jax.random.permutation(keys[1 + section], M)
        field = field[order]
        raw = jax.random.normal(keys[4 + section], (M // group, group, group), jnp.float32)
        rotation, upper = jnp.linalg.qr(raw)
        field = jnp.einsum('gij,gjk->gik', rotation, field.reshape(M // group, group, K), precision=lax.Precision.HIGHEST).reshape(M, K)
    lowest = 0.8
    column_scale = jnp.exp(jax.random.uniform(keys[7], (1, K), jnp.float32, math.log(lowest), -math.log(lowest)))
    tilt = min(0.0015 * math.sqrt(M), 0.4)
    drift = jax.random.truncated_normal(jax.random.fold_in(key, 11), -4.0, 4.0, (M, K), jnp.float32)
    return field * math.sqrt(M) * column_scale + tilt * drift


def draw_block(key, part):
    keys = jax.random.split(key, 2)
    normal_part = jax.random.truncated_normal(keys[0], -4.0, 4.0, (M, NBLK * BLK), jnp.float32)
    position = jnp.arange(M, dtype=jnp.float32) / M
    row_scale = jnp.exp(math.log(3.0) * position + math.log(10.0) * jax.random.uniform(keys[1], (M,), jnp.float32))
    return normal_part * row_scale[:, None]


def setup_inputs(seed: int = 0) -> dict:
    key_list = jax.random.split(jax.random.key(seed), 3)
    return {
        "basis": draw_basis(jax.random.fold_in(key_list[2], 71), 0),
        "block": draw_block(jax.random.fold_in(key_list[2], 71), 0),
    }


def solve_block(lower_factor, vectors):
    return jax.scipy.linalg.solve_triangular(lower_factor, vectors, lower=True)

def reference(basis, block):
    highest = lax.Precision.HIGHEST
    coef_one = jnp.dot(basis.T.astype(jnp.float32), block.astype(jnp.float32), precision=highest, preferred_element_type=jnp.float32) / M
    first = block - jnp.dot(basis.astype(jnp.float32), coef_one.astype(jnp.float32), precision=highest, preferred_element_type=jnp.float32)
    coef_two = jnp.dot(basis.T.astype(jnp.float32), first.astype(jnp.float32), precision=highest, preferred_element_type=jnp.float32) / M
    second = first - jnp.dot(basis.astype(jnp.float32), coef_two.astype(jnp.float32), precision=highest, preferred_element_type=jnp.float32)
    pieces = second.reshape(M, NBLK, BLK)
    gram = jnp.einsum('mbi,mbj->bij', pieces, pieces, precision=highest) / M
    lower_factor = jnp.linalg.cholesky(gram)
    solved = jax.vmap(solve_block)(lower_factor, jnp.transpose(pieces, (1, 2, 0)))
    ortho = jnp.transpose(solved, (2, 0, 1)).reshape(M, NBLK * BLK)
    return (ortho, jnp.transpose(lower_factor, (0, 2, 1)))
```

```python
import functools

import jax
import jax.numpy as jnp
from jax import lax
from jax.sharding import PartitionSpec as P

BLK = 128
CHUNKS = 2
HIGH = lax.Precision.HIGH
HIGHEST = lax.Precision.HIGHEST


def swap(value, axis, mask):
    count = lax.axis_size(axis)
    return lax.ppermute(value, axis, [(i, i ^ mask) for i in range(count)])


def radices(count):
    sizes = []
    while count > 1:
        size = 4 if count % 4 == 0 else 2
        sizes.append(size)
        count //= size
    return sizes


def sum_rows(value, sizes):
    if len(sizes) == 0:
        return value
    return sum_stage(value, sizes, 1)


def sum_stage(value, sizes, stride):
    size = sizes[0]
    if len(sizes) == 1:
        got = [swap(value, "rows", k * stride) for k in range(1, size)]
        for other in got:
            value = value + other
        return value
    part = value.shape[0] // size
    pieces = [value[k * part : (k + 1) * part] for k in range(size)]
    got = [swap(pieces[k], "rows", k * stride) for k in range(1, size)]
    own = pieces[0]
    for other in got:
        own = own + other
    own = sum_stage(own, sizes[1:], stride * size)
    return jnp.concatenate([own] + [swap(own, "rows", k * stride) for k in range(1, size)], 0)


def body(basis, block):
    rows = lax.axis_size("rows")
    sizes = radices(rows)
    split = 1
    for size in sizes[:-1]:
        split *= size
    inverse = 1.0 / (basis.shape[0] * rows)
    others = lax.axis_size("cols") // 2
    index = lax.axis_index("rows") % split
    part = basis.shape[1] // split

    mate = swap(basis, "cols", 1)

    def block_at(place):
        mask, stride, rest = 0, 1, place
        width = split
        for size in sizes[:-1]:
            width //= size
            digit, rest = rest // width, rest % width
            mask += digit * stride
            stride *= size
        return (index ^ mask) * part

    wide = []
    for place in range(split):
        start = block_at(place)
        wide += [lax.dynamic_slice_in_dim(t, start, part, 1) for t in (basis, mate)]
    wide = jnp.concatenate(wide, 1)

    def project(piece):
        return lax.dot_general(
            wide, piece, (((0,), (0,)), ((), ())), precision=HIGH, preferred_element_type=jnp.float32
        ) * inverse

    def expand(coef):
        return jnp.dot(wide, coef, precision=HIGH, preferred_element_type=jnp.float32)

    step = block.shape[1] // CHUNKS

    def run(own):
        width = own.shape[1]
        vectors = jnp.concatenate([own] + [swap(own, "cols", 2 * j) for j in range(1, others)], 1)
        coef_one = sum_rows(project(vectors), sizes)
        shift = expand(coef_one)
        total = shift
        for j in range(1, others):
            other = swap(shift, "cols", 2 * j).reshape(-1, others, width)
            order = [k ^ j for k in range(others)]
            total = total + jnp.concatenate([other[:, k] for k in order], 1)
        first = vectors - total
        coef_two = sum_rows(project(first), sizes)
        again = expand(coef_two)
        second = first[:, :width] - again[:, :width]
        for j in range(1, others):
            second = second - swap(again[:, j * width : (j + 1) * width], "cols", 2 * j)
        return second

    second = jnp.concatenate([run(block[:, c * step : (c + 1) * step]) for c in range(CHUNKS)], 1)
    blocks = second.shape[1] // BLK
    pieces = second.reshape(-1, blocks, BLK)
    gram = jnp.einsum("mbi,mbj->bij", pieces, pieces, precision=HIGHEST) * inverse
    stride = 1
    for size in sizes:
        for other in [swap(gram, "rows", k * stride) for k in range(1, size)]:
            gram = gram + other
        stride *= size
    lower = jnp.linalg.cholesky(gram)
    eye = jnp.broadcast_to(jnp.eye(BLK, dtype=jnp.float32), lower.shape)
    inv = jax.vmap(functools.partial(jax.scipy.linalg.solve_triangular, lower=True))(lower, eye)
    ortho = jnp.einsum("mbi,bji->mbj", pieces, inv, precision=HIGHEST).reshape(second.shape)
    return ortho, jnp.transpose(lower, (0, 2, 1))


def solution(mesh):
    spec = P("rows", "cols")
    return jax.shard_map(
        body, mesh=mesh, in_specs=(spec, spec), out_specs=(spec, P("cols", None, None)), check_vma=False
    )
```

```python
import jax
import jax.numpy as jnp
from jax import lax
from jax.experimental import pallas as pl
from jax.experimental.pallas import tpu as pltpu
from jax.sharding import PartitionSpec as P

BLK = 128
CHUNKS = 2
HIGHEST = lax.Precision.HIGHEST
F32 = jnp.float32
BF16 = jnp.bfloat16


def swap(value, axis, mask):
    count = lax.axis_size(axis)
    return lax.ppermute(value, axis, [(i, i ^ mask) for i in range(count)])


def radices(count):
    sizes = []
    while count > 1:
        size = 4 if count % 4 == 0 else 2
        sizes.append(size)
        count //= size
    return sizes


def sum_rows(value, sizes, stride=1):
    if len(sizes) == 0:
        return value
    size = sizes[0]
    if len(sizes) == 1:
        for other in [swap(value, "rows", k * stride) for k in range(1, size)]:
            value = value + other
        return value
    part = value.shape[0] // size
    pieces = [value[k * part : (k + 1) * part] for k in range(size)]
    own = pieces[0]
    for other in [swap(pieces[k], "rows", k * stride) for k in range(1, size)]:
        own = own + other
    own = sum_rows(own, sizes[1:], stride * size)
    return jnp.concatenate([own] + [swap(own, "rows", k * stride) for k in range(1, size)], 0)


def halves(value):
    high = lax.reduce_precision(value, 8, 7)
    return high.astype(BF16), (value - high).astype(BF16)


def prepare_kernel(places_ref, own_ref, mate_ref, high_ref, low_ref):
    width = own_ref.shape[1]
    for side, ref in enumerate((own_ref, mate_ref)):
        value = ref[...]
        high = value.astype(BF16)
        high_ref[:, side * width : (side + 1) * width] = high
        low_ref[:, side * width : (side + 1) * width] = (value - high.astype(F32)).astype(BF16)


def prepare(own, mate, places):
    height, width = own.shape
    split = len(places)
    part = width // split
    if part % 128 != 0:
        blocks = [lax.dynamic_slice_in_dim(t, p * part, part, 1) for p in places for t in (own, mate)]
        return halves(jnp.concatenate(blocks, 1))
    rows = height // 2
    piece = pl.BlockSpec((rows, part), lambda p, r, places: (r, places[p]))
    wide = pl.BlockSpec((rows, 2 * part), lambda p, r, places: (r, p))
    return pl.pallas_call(
        prepare_kernel,
        grid_spec=pltpu.PrefetchScalarGridSpec(
            num_scalar_prefetch=1, grid=(split, 2), in_specs=[piece, piece], out_specs=[wide, wide]
        ),
        out_shape=[jax.ShapeDtypeStruct((height, 2 * width), BF16)] * 2,
        name="prepare",
    )(jnp.stack(places).astype(jnp.int32), own, mate)


def factor_kernel(gram_ref, second_ref, ortho_ref, upper_ref):
    n = gram_ref.shape[0]
    groups = n // 8
    sub = lax.broadcasted_iota(jnp.int32, (8, n), 0)
    lane = lax.broadcasted_iota(jnp.int32, (8, n), 1)

    def spread(value, i):
        return jnp.broadcast_to(value[i : i + 1, :], (8, n))

    def column(value, i):
        return jnp.broadcast_to(value[:, i : i + 1], (8, n))

    left = [gram_ref[8 * g : 8 * g + 8, :] for g in range(groups)]
    right = [jnp.where(lane == sub + 8 * g, 1.0, 0.0) for g in range(groups)]
    for g in range(groups):
        a, v = left[g], right[g]
        cols = [column(a, 8 * g + k) for k in range(8)]
        roots, rows_a, rows_v, factors = [], [], [], []
        for i in range(8):
            pivot = spread(cols[i], i)
            root = lax.rsqrt(pivot)
            root = root * (1.5 - (0.5 * pivot * root) * root)
            u = cols[i] * root
            splat = {k: spread(u, k) for k in range(i + 1, 8)}
            for k in range(i + 1, 8):
                cols[k] = cols[k] - u * splat[k]
            row_a, row_v = spread(a, i) * root, spread(v, i) * root
            below = jnp.where(sub > i, u, 0.0)
            a = jnp.where(sub == i, row_a, a - below * row_a)
            v = jnp.where(sub == i, row_v, v - below * row_v)
            roots.append(root)
            rows_a.append(row_a)
            rows_v.append(row_v)
            factors.append(splat)
        left[g], right[g] = a, v
        for h in range(g + 1, groups):
            raw = left[h]
            mults = []
            a, v = raw, right[h]
            for i in range(8):
                m = column(raw, 8 * g + i)
                for k in range(i):
                    m = m - factors[k][i] * mults[k]
                m = m * roots[i]
                mults.append(m)
                a = a - m * rows_a[i]
                v = v - m * rows_v[i]
            left[h], right[h] = a, v
    for g in range(groups):
        upper_ref[8 * g : 8 * g + 8, :] = jnp.where(lane >= sub + 8 * g, left[g], 0.0)
    ortho_ref[...] = lax.dot_general(
        second_ref[...],
        jnp.concatenate(right, 0),
        (((1,), (1,)), ((), ())),
        precision=HIGHEST,
        preferred_element_type=F32,
    )


def factor(gram, second):
    return pl.pallas_call(
        factor_kernel,
        out_shape=[jax.ShapeDtypeStruct(second.shape, F32), jax.ShapeDtypeStruct(gram.shape, F32)],
        name="factor",
    )(gram, second)


def body(basis, block):
    rows = lax.axis_size("rows")
    sizes = radices(rows)
    split = 1
    for size in sizes[:-1]:
        split *= size
    inverse = 1.0 / (basis.shape[0] * rows)
    others = lax.axis_size("cols") // 2
    index = lax.axis_index("rows") % split

    def mask_of(place):
        mask, stride, width = 0, 1, split
        for size in sizes[:-1]:
            width //= size
            mask += (place // width) * stride
            place, stride = place % width, stride * size
        return mask

    mate = swap(basis, "cols", 1)
    peers = [block] + [swap(block, "cols", 2 * j) for j in range(1, others)]
    high, low = prepare(basis, mate, [index ^ mask_of(p) for p in range(split)])

    def times(left, right, dims):
        pair = jnp.concatenate(halves(right), 1)
        both = lax.dot_general(left[0], pair, (dims, ((), ())), preferred_element_type=F32)
        both = both + lax.dot_general(left[1], pair, (dims, ((), ())), preferred_element_type=F32)
        return both[:, : right.shape[1]] + both[:, right.shape[1] :]

    def project(piece):
        return times((high, low), piece * inverse, ((0,), (0,)))

    def expand(coef):
        return times((high, low), coef, ((1,), (0,)))

    def pack(value):
        half = value.shape[0] // 2
        return jnp.concatenate([value[:half], value[half:]], 1)

    def unpack(value):
        half = value.shape[1] // 2
        return jnp.concatenate([value[:, :half], value[:, half:]], 0)

    width = block.shape[1] // CHUNKS

    def run(chunk):
        vectors = jnp.concatenate([p[:, chunk * width : (chunk + 1) * width] for p in peers], 1)
        coef_one = sum_rows(project(vectors), sizes)
        shift = expand(coef_one)
        total = shift
        for j in range(1, others):
            other = swap(shift, "cols", 2 * j)
            total = total + jnp.concatenate(
                [other[:, (k ^ j) * width : ((k ^ j) + 1) * width] for k in range(others)], 1
            )
        first = vectors - total
        coef_two = sum_rows(project(first), sizes)
        again = expand(coef_two)
        second = first[:, :width] - again[:, :width]
        for j in range(1, others):
            second = second - unpack(swap(pack(again[:, j * width : (j + 1) * width]), "cols", 2 * j))
        return second

    second = jnp.concatenate([run(c) for c in range(CHUNKS)], 1)
    orthos, uppers = [], []
    for b in range(second.shape[1] // BLK):
        piece = second[:, b * BLK : (b + 1) * BLK]
        gram = lax.dot_general(piece, piece, (((0,), (0,)), ((), ())), precision=HIGHEST) * inverse
        stride = 1
        for size in sizes:
            for other in [swap(gram, "rows", k * stride) for k in range(1, size)]:
                gram = gram + other
            stride *= size
        ortho, upper = factor(gram, piece)
        orthos.append(ortho)
        uppers.append(upper)
    return jnp.concatenate(orthos, 1), jnp.stack(uppers)


def solution(mesh):
    spec = P("rows", "cols")
    return jax.shard_map(
        body, mesh=mesh, in_specs=(spec, spec), out_specs=(spec, P("cols", None, None)), check_vma=False
    )
```

```python
import jax
import jax.numpy as jnp
from jax import lax
from jax.experimental import pallas as pl
from jax.experimental.pallas import tpu as pltpu
from jax.sharding import PartitionSpec as P

BLK = 128
CHUNKS = 2
HIGHEST = lax.Precision.HIGHEST
F32 = jnp.float32
BF16 = jnp.bfloat16
VMEM = pl.BlockSpec(memory_space=pltpu.VMEM)
SMEM = pl.BlockSpec(memory_space=pltpu.SMEM)
ANY = pl.BlockSpec(memory_space=pl.ANY)
DOWN = (((0,), (0,)), ((), ()))
ACROSS = (((1,), (0,)), ((), ()))


def swap(value, axis, mask):
    count = lax.axis_size(axis)
    return lax.ppermute(value, axis, [(i, i ^ mask) for i in range(count)])


def radices(count):
    sizes = []
    while count > 1:
        size = 4 if count % 4 == 0 else 2
        sizes.append(size)
        count //= size
    return sizes


def call(kernel, name, shapes, args, flops=0, specs=None, after=()):
    specs = [VMEM] * len(args) if specs is None else specs
    used = len(args)

    def run(*refs):
        kernel(*refs[:used], *refs[used + len(after) :])

    return pl.pallas_call(
        run,
        out_shape=[jax.ShapeDtypeStruct(s, t) for s, t in shapes],
        in_specs=list(specs) + [ANY] * len(after),
        out_specs=[VMEM] * len(shapes),
        compiler_params=pltpu.CompilerParams(vmem_limit_bytes=12 * 1024 * 1024),
        cost_estimate=pl.CostEstimate(flops=int(flops), transcendentals=0, bytes_accessed=0),
        name=name,
    )(*args, *after)


def halves(value):
    high = value.astype(BF16)
    return jnp.concatenate([high, (value - high.astype(F32)).astype(BF16)], 1)


def fold(value):
    width = value.shape[1] // 2
    return value[:, :width] + value[:, width:]


def prepare_kernel(places_ref, tile_ref, high_ref, low_ref, *, split):
    part = tile_ref.shape[1] // split
    for p in range(split):
        start = pl.multiple_of(places_ref[p] * part, part)
        value = tile_ref[:, pl.ds(start, part)]
        high = value.astype(BF16)
        high_ref[:, p * part : (p + 1) * part] = high
        low_ref[:, p * part : (p + 1) * part] = (value - high.astype(F32)).astype(BF16)


def prepare(tile, places, split):
    def kernel(*refs):
        prepare_kernel(*refs, split=split)

    return call(kernel, "prepare", [(tile.shape, BF16)] * 2, [places, tile], 2e8, [SMEM, VMEM])


def pack(value):
    half = value.shape[0] // 2
    return jnp.concatenate([value[:half], value[half:]], 1)


def unpack(value):
    half = value.shape[1] // 2
    return jnp.concatenate([value[:, :half], value[:, half:]], 0)


def project_into(vectors, tiles, pieces):
    pair = halves(vectors)
    part = tiles[0][0].shape[1] // len(pieces)
    for p, piece in enumerate(pieces):
        for s, (high, low) in enumerate(tiles):
            both = lax.dot_general(high[:, p * part : (p + 1) * part], pair, DOWN, preferred_element_type=F32)
            both = both + lax.dot_general(low[:, p * part : (p + 1) * part], pair, DOWN, preferred_element_type=F32)
            piece[s * part : (s + 1) * part, :] = fold(both)


def expand_rows(pieces, tiles):
    part = tiles[0][0].shape[1] // len(pieces)
    pairs = [
        jnp.concatenate([halves(piece[s * part : (s + 1) * part, :]) for piece in pieces], 0)
        for s in range(len(tiles))
    ]
    height = tiles[0][0].shape[0]
    step = min(256, height)
    for start in range(0, height, step):
        rows = slice(start, start + step)
        both = None
        for (high, low), pair in zip(tiles, pairs):
            for ref in (high, low):
                term = lax.dot_general(ref[rows, :], pair, ACROSS, preferred_element_type=F32)
                both = term if both is None else both + term
        yield rows, fold(both)


def factor_kernel(gram_a_ref, gram_b_ref, second_ref, ortho_ref, upper_ref):
    n = gram_a_ref.shape[0]
    groups = n // 8
    sub = lax.broadcasted_iota(jnp.int32, (8, n), 0)
    lane = lax.broadcasted_iota(jnp.int32, (8, n), 1)

    def spread(value, i):
        return jnp.broadcast_to(value[i : i + 1, :], (8, n))

    def column(value, i):
        return jnp.broadcast_to(value[:, i : i + 1], (8, n))

    left = [gram_a_ref[8 * g : 8 * g + 8, :] + gram_b_ref[8 * g : 8 * g + 8, :] for g in range(groups)]
    right = [jnp.where(lane == sub + 8 * g, 1.0, 0.0) for g in range(groups)]
    for g in range(groups):
        a, v = left[g], right[g]
        cols = [column(a, 8 * g + k) for k in range(8)]
        roots, rows_a, rows_v, factors = [], [], [], []
        for i in range(8):
            pivot = spread(cols[i], i)
            root = lax.rsqrt(pivot)
            root = root * (1.5 - (0.5 * pivot * root) * root)
            u = cols[i] * root
            splat = {k: spread(u, k) for k in range(i + 1, 8)}
            for k in range(i + 1, 8):
                cols[k] = cols[k] - u * splat[k]
            row_a, row_v = spread(a, i) * root, spread(v, i) * root
            below = jnp.where(sub > i, u, 0.0)
            a = jnp.where(sub == i, row_a, a - below * row_a)
            v = jnp.where(sub == i, row_v, v - below * row_v)
            roots.append(root)
            rows_a.append(row_a)
            rows_v.append(row_v)
            factors.append(splat)
        left[g], right[g] = a, v
        for h in range(g + 1, groups):
            raw = left[h]
            mults = []
            a, v = raw, right[h]
            for i in range(8):
                m = column(raw, 8 * g + i)
                for k in range(i):
                    m = m - factors[k][i] * mults[k]
                m = m * roots[i]
                mults.append(m)
                a = a - m * rows_a[i]
                v = v - m * rows_v[i]
            left[h], right[h] = a, v
    for g in range(groups):
        upper_ref[8 * g : 8 * g + 8, :] = jnp.where(lane >= sub + 8 * g, left[g], 0.0)
    ortho_ref[...] = lax.dot_general(
        second_ref[...],
        jnp.concatenate(right, 0),
        (((1,), (1,)), ((), ())),
        precision=HIGHEST,
        preferred_element_type=F32,
    )


def body(basis, block):
    rows = lax.axis_size("rows")
    sizes = radices(rows)
    split = sizes[0] if sizes else 1
    height, columns = basis.shape
    inverse = 1.0 / (height * rows)
    others = lax.axis_size("cols") // 2
    index = lax.axis_index("rows") % split
    places = jnp.stack([index ^ p for p in range(split)]).astype(jnp.int32)
    width = block.shape[1] // CHUNKS
    wide = others * width
    coef_shape = (2 * columns // split, wide)
    vector_shape = (height, wide)
    work = 2 * height * 2 * columns * wide

    def pack_kernel(block_ref, *refs):
        for c, ref in enumerate(refs):
            ref[...] = pack(block_ref[:, c * width : (c + 1) * width])

    mate = swap(basis, "cols", 1)
    packed = call(pack_kernel, "pack", [((height // 2, 2 * width), F32)] * CHUNKS, [block], 1e7)
    others_in = [[swap(p, "cols", 2 * j) for j in range(1, others)] for p in packed]
    tiles = prepare(basis, places, split) + prepare(mate, places, split)

    def grouped(refs):
        return [(refs[0], refs[1]), (refs[2], refs[3])]

    def exchange(pieces):
        own = pieces[0]
        for other in [swap(pieces[k], "rows", k) for k in range(1, split)]:
            own = own + other
        stride = split
        for size in sizes[1:]:
            for other in [swap(own, "rows", k * stride) for k in range(1, size)]:
                own = own + other
            stride *= size
        return [own] + [swap(own, "rows", k) for k in range(1, split)]

    def start(c):
        def kernel(block_ref, *refs):
            got, refs = refs[: others - 1], refs[others - 1 :]
            basis_refs, vector_ref, pieces = refs[:4], refs[4], refs[5:]
            vectors = [block_ref[:, c * width : (c + 1) * width]] + [unpack(ref[...]) for ref in got]
            vectors = jnp.concatenate(vectors, 1)
            vector_ref[...] = vectors
            project_into(vectors * inverse, grouped(basis_refs), pieces)

        shapes = [(vector_shape, F32)] + [(coef_shape, F32)] * split
        out = call(kernel, "start", shapes, [block, *others_in[c], *tiles], work)
        return out[0], out[1:]

    def shift(pieces):
        def kernel(*refs):
            coefs, basis_refs, out_ref = refs[:split], refs[split : split + 4], refs[split + 4]
            for where, value in expand_rows(coefs, grouped(basis_refs)):
                out_ref[where, :] = value

        return call(kernel, "shift", [(vector_shape, F32)], [*pieces, *tiles], work)[0]

    def again(vectors, own, got):
        def kernel(vector_ref, own_ref, *refs):
            got_refs, refs = refs[: others - 1], refs[others - 1 :]
            basis_refs, first_ref, pieces = refs[:4], refs[4], refs[5:]
            first = vector_ref[...] - own_ref[...]
            for j, ref in enumerate(got_refs, 1):
                first = first - jnp.concatenate(
                    [ref[:, (k ^ j) * width : ((k ^ j) + 1) * width] for k in range(others)], 1
                )
            first_ref[...] = first
            project_into(first * inverse, grouped(basis_refs), pieces)

        shapes = [(vector_shape, F32)] + [(coef_shape, F32)] * split
        out = call(kernel, "again", shapes, [vectors, own, *got, *tiles], work)
        return out[0], out[1:]

    def finish(pieces, first):
        def kernel(*refs):
            coefs, first_ref, basis_refs = refs[:split], refs[split], refs[split + 1 : split + 5]
            own_ref, sends = refs[split + 5], refs[split + 6 :]
            step = None
            for where, value in expand_rows(coefs, grouped(basis_refs)):
                own_ref[where, :] = first_ref[where, :width] - value[:, :width]
                side, top = divmod(where.start, height // 2)
                for j, ref in enumerate(sends, 1):
                    ref[top : top + value.shape[0], side * width : (side + 1) * width] = value[
                        :, j * width : (j + 1) * width
                    ]

        shapes = [((height, width), F32)] + [((height // 2, 2 * width), F32)] * (others - 1)
        out = call(kernel, "finish", shapes, [*pieces, first, *tiles], work)
        return out[0], [swap(value, "cols", 2 * j) for j, value in enumerate(out[1:], 1)]

    def run(c):
        vectors, pieces = start(c)
        own = shift(exchange(pieces))
        first, pieces = again(vectors, own, [swap(own, "cols", 2 * j) for j in range(1, others)])
        return finish(exchange(pieces), first)

    parts = [run(c) for c in range(CHUNKS)]

    def gram_kernel(*refs):
        second_ref, gram_ref = refs[-2:]
        for c in range(CHUNKS):
            own_ref, *got = refs[c * others : (c + 1) * others]
            value = own_ref[...]
            for ref in got:
                value = value - unpack(ref[...])
            second_ref[:, c * width : (c + 1) * width] = value
        second = second_ref[...]
        gram_ref[...] = lax.dot_general(second, second, DOWN, precision=HIGHEST, preferred_element_type=F32) * inverse

    args = [a for own, got in parts for a in (own, *got)]
    second, gram = call(gram_kernel, "gram", [(block.shape, F32), ((BLK, BLK), F32)], args, work // 4)
    terms = [gram]
    stride = 1
    for size in sizes:
        gram = sum(terms[1:], terms[0])
        terms = [gram] + [swap(gram, "rows", k * stride) for k in range(1, size)]
        stride *= size
    last = sum(terms[1:-1], terms[0]) if len(terms) > 1 else terms[0]
    other = terms[-1] if len(terms) > 1 else jnp.zeros_like(last)
    ortho, upper = call(factor_kernel, "factor", [(block.shape, F32), ((BLK, BLK), F32)], [last, other, second], work)
    return ortho, upper[None]


def solution(mesh):
    spec = P("rows", "cols")
    return jax.shard_map(
        body, mesh=mesh, in_specs=(spec, spec), out_specs=(spec, P("cols", None, None)), check_vma=False
    )
```
